32 devices in a mesh: gx: 8 (over y, x, core), gy: 4 (over z).
Axes of the slice: x: 2, y: 2, z: 4, core: 2. Of those that a mesh axis runs over, the one named last changes fastest.
Arguments:
- cells: int32 [3, 1048576], P(None, ('gx', 'gy')), may hold values from 0 to 255, as said below
- fractions: float32 [3, 1048576], P(None, ('gx', 'gy')), may hold values from 0 to 1
- charges: float32 [1048576], P(('gx', 'gy')), may hold values from -24 to 24
- influence: float32 [256, 256, 256], P('gx', 'gy'), may hold values from 0.05 to 24, as said below
- shells: int32 [256, 256, 256], P('gx', 'gy'), may hold values from 0 to 255
Outputs:
- potential_hat: float32 [2, 256, 256, 256], P(None, 'gx', 'gy')
- energy: float32 [], replicated
- virial: float32 [3, 3], replicated
- spectrum: float32 [256], replicated
The draws below stay inside these ranges and needn't reach their ends.
Inputs may be any that keep to these rules, and one draw needn't show every extreme that they name: `cells`: atom a belongs to device a // 32768, devices numbered with gy fastest; its y cell lies in that device's block of 32 y planes (block index its gx index) and its z cell in its block of 64 z planes (block index its gy index). `influence`: Positive.
All inputs are finite; a program needn't handle non-finite values.
Results may differ from the reference program's by a relative error of at most 0.0029.
Values sent between devices are 32-bit elements; how exact they have to be, the bound alone decides.
A program may use at most 64 MiB of HBM per device.

```python
import jax
import jax.numpy as jnp
from jax import lax

MESH = 256
SHELLS = 256
SCREEN = 4096
ATOM_DEV = 32768
ATOMS = 1048576
CYD = 32
CZD = 64


def draw_cells(key, part):
    keys = jax.random.split(jax.random.fold_in(key, 11), 3)
    row_index = jnp.arange(ATOMS, dtype=jnp.int32)
    device = row_index // ATOM_DEV
    columns = MESH // CZD
    cell_x = jax.random.randint(keys[0], (ATOMS,), 0, MESH, dtype=jnp.int32)
    cell_y = device // columns * CYD + jax.random.randint(keys[1], (ATOMS,), 0, CYD, dtype=jnp.int32)
    cell_z = device % columns * CZD + jax.random.randint(keys[2], (ATOMS,), 0, CZD, dtype=jnp.int32)
    return jnp.stack([cell_x, cell_y, cell_z]).astype(jnp.int32)


def wave_squared():
    index = jnp.arange(MESH, dtype=jnp.int32)
    wave = jnp.where(index < MESH // 2, index, index - MESH).astype(jnp.float32)
    return wave[:, None, None] ** 2 + wave[None, :, None] ** 2 + wave[None, None, :] ** 2


def draw_influence(key, part):
    squared = wave_squared()
    shape = (MESH, MESH, MESH)
    rough = jnp.exp(jax.random.uniform(jax.random.fold_in(key, 22), shape, jnp.float32, -0.6931, 0.6931))
    return (rough * 8.0 / (1.0 + squared / 2048.0)).astype(jnp.float32)


def draw_shells(key, part):
    metric_tensor = jax.random.randint(jax.random.fold_in(key, 31), (3,), 1, 4, dtype=jnp.int32)
    index = jnp.arange(MESH, dtype=jnp.int32)
    wave = jnp.where(index < MESH // 2, index, index - MESH)
    radius = metric_tensor[0] * wave[:, None, None] ** 2 + metric_tensor[1] * wave[None, :, None] ** 2 + metric_tensor[2] * wave[None, None, :] ** 2
    top_value = (metric_tensor[0] + metric_tensor[1] + metric_tensor[2]) * (MESH // 2) ** 2
    return jnp.minimum(radius * SHELLS // (top_value + 1), SHELLS - 1).astype(jnp.int32)


def block_levels(rng, dims, pieces, smallest, largest):
    def one(dim, parts):
        steps = jax.random.uniform(jax.random.fold_in(jax.random.fold_in(rng, 6), dim), (parts,), jnp.float32, smallest / len(pieces), largest / len(pieces))
        return jnp.repeat(jnp.exp(steps), dims[dim] // parts).reshape((-1,) + (1,) * (len(dims) - dim - 1))

    level = one(*pieces[0])
    for cut in pieces[1:]:
        level = level * one(*cut)
    return level


def centred(rng, shape, width, most, pieces=(), kind=jnp.bfloat16):
    factor_of = block_levels(rng, shape, pieces, -0.22, 0.18) if pieces else 1.0
    values = jax.random.normal(rng, shape, jnp.float32) * width * factor_of
    return jnp.minimum(jnp.maximum(values, -most), most).astype(kind)


def setup_inputs(seed: int = 0) -> dict:
    splits = jax.random.split(jax.random.key(seed), 6)
    return {
        "cells": draw_cells(jax.random.fold_in(splits[5], 71), 0),
        "fractions": jnp.clip(1.0 * jax.random.uniform(splits[1], (3, ATOMS), jnp.float32) ** block_levels(splits[1], (3, ATOMS), ((1, 32),), -0.2, 0.2), 0.0, 1.0),
        "charges": centred(splits[2], (ATOMS,), 4.0, 24.0, ((0, 32),), jnp.float32),
        "influence": draw_influence(jax.random.fold_in(splits[5], 71), 0),
        "shells": draw_shells(jax.random.fold_in(splits[5], 71), 0),
    }


def spline(frac):
    cube = frac * frac * frac
    square = frac * frac
    rest = 1.0 - frac
    return (rest * rest * rest / 6.0, (3.0 * cube - 6.0 * square + 4.0) / 6.0, (-3.0 * cube + 3.0 * square + 3.0 * frac + 1.0) / 6.0, cube / 6.0)


def wave_numbers(index):
    return jnp.where(index < MESH // 2, index, index - MESH).astype(jnp.float32)


def reference(cells, fractions, charges, influence, shells):
    weight_x = spline(fractions[0])
    weight_y = spline(fractions[1])
    weight_z = spline(fractions[2])
    charge_mesh = jnp.zeros((MESH, MESH, MESH), jnp.float32)
    for first in range(4):
        factor_x = lax.optimization_barrier((charges * weight_x[first]).astype(jnp.bfloat16)).astype(jnp.float32)
        index_x = ((cells[0] + first) % MESH).astype(jnp.int32)
        for second in range(4):
            index_y = ((cells[1] + second) % MESH).astype(jnp.int32)
            for third in range(4):
                index_z = ((cells[2] + third) % MESH).astype(jnp.int32)
                factor_yz = lax.optimization_barrier((weight_y[second] * weight_z[third]).astype(jnp.bfloat16)).astype(jnp.float32)
                charge_mesh = charge_mesh.at[index_x, index_y, index_z].add(factor_x * factor_yz)
    transform = jnp.fft.fftn(charge_mesh) / (MESH ** 1.5)
    real_part = jnp.real(transform).astype(jnp.float32)
    imag_part = jnp.imag(transform).astype(jnp.float32)
    index = jnp.arange(MESH, dtype=jnp.int32)
    wave = wave_numbers(index)
    wave_x = wave[:, None, None]
    wave_y = wave[None, :, None]
    wave_z = wave[None, None, :]
    squared = wave_x * wave_x + wave_y * wave_y + wave_z * wave_z
    keep = jnp.where(squared > 0.0, 1.0, 0.0).astype(jnp.float32)
    weight = keep * influence
    potential_hat = jnp.stack([weight * real_part, weight * imag_part])
    power = real_part * real_part + imag_part * imag_part
    influence_weighted = weight * power
    scale = 0.5 / (MESH ** 3)
    whole_sum = jnp.sum(influence_weighted)
    energy = scale * whole_sum
    coef = influence_weighted * 2.0 * (1.0 + squared / SCREEN) / (squared + 1.0 - keep)
    waves = (wave_x, wave_y, wave_z)
    rows_out = []
    for left in range(3):
        entries = []
        for right in range(3):
            cross = jnp.sum(coef * waves[left] * waves[right])
            diagonal = whole_sum if left == right else jnp.float32(0.0)
            entries.append(scale * (diagonal - cross))
        rows_out.append(jnp.stack(entries))
    virial = jnp.stack(rows_out)
    spectrum = jax.ops.segment_sum(power.reshape(-1), shells.reshape(-1).astype(jnp.int32), num_segments=SHELLS) * (SHELLS / (MESH ** 3))
    return potential_hat, energy, virial, spectrum
```

```python
import functools
import math

import jax
import jax.numpy as jnp
import numpy as np
from jax import lax
from jax.experimental import pallas as pl
from jax.experimental.pallas import tpu as pltpu
from jax.sharding import PartitionSpec as P

MESH = 256
SHELLS = 256
SCREEN = 4096
HALO_Y = 4
HALO_Z = 3
PLANES = 8
GROUP = 4
BLOCK = 1024
SUBS = 8
FIRST_SUBS = 4
BUFFERS = 4
PACK = 16
SIXTH = 1.0 / 6.0
AHEAD = (9, 9, 7, 1)
NT = (((1,), (1,)), ((), ()))
NN = (((1,), (0,)), ((), ()))


def spline(frac):
    cube = frac * frac * frac
    square = frac * frac
    rest = 1.0 - frac
    return (
        rest * rest * rest * SIXTH,
        (3.0 * cube - 6.0 * square + 4.0) * SIXTH,
        (-3.0 * cube + 3.0 * square + 3.0 * frac + 1.0) * SIXTH,
        cube * SIXTH,
    )


def split(values):
    high = values.astype(jnp.bfloat16)
    low = (values - high.astype(jnp.float32)).astype(jnp.bfloat16)
    return high, low


def dot(left, right, dims):
    return lax.dot_general(left, right, dims, preferred_element_type=jnp.float32)


def dot3(left, right, dims):
    return (
        dot(left[0], right[0], dims) + dot(left[0], right[1], dims) + dot(left[1], right[0], dims)
    )


def table_pair(table):
    high = jnp.asarray(table.astype(np.float32)).astype(jnp.bfloat16)
    low = jnp.asarray(
        (table - table.astype(np.float32).astype(jnp.bfloat16).astype(np.float64)).astype(np.float32)
    ).astype(jnp.bfloat16)
    return high, low


def wave_tables():
    index = np.arange(MESH)
    angle = (index[:, None] * index[None, :] % MESH) * (2.0 * math.pi / MESH)
    factor = 1.0 / math.sqrt(MESH)
    return np.cos(angle) * factor, np.sin(angle) * factor


def wave_numbers(index):
    return jnp.where(index < MESH // 2, index, index - MESH).astype(jnp.float32)


def tiles_of(cell, weights, rows, kind):
    shape = (rows, cell.shape[1])
    row = lax.broadcasted_iota(jnp.int32, shape, 0)
    low = cell & (rows - 1)
    shift = (row - low) & (rows - 1)
    value = jnp.zeros(shape, jnp.float32)
    for offset in range(4):
        value = jnp.where(shift == offset, weights[offset], value)
    tile = (cell // rows) + jnp.where(row < low, 1, 0)
    return value.astype(kind), tile


def tables():
    cosine, sine = wave_tables()
    along_x = np.concatenate([cosine, -sine], axis=0)
    return cosine, sine, along_x


def table_y(cosine, sine, parts_z):
    rows = MESH // parts_z
    table = np.zeros((2, MESH, parts_z, max(2 * rows, 128)))
    cosine = cosine.reshape(MESH, parts_z, rows)
    sine = sine.reshape(MESH, parts_z, rows)
    table[0, :, :, :rows] = cosine
    table[0, :, :, rows : 2 * rows] = -sine
    table[1, :, :, :rows] = sine
    table[1, :, :, rows : 2 * rows] = cosine
    return table.reshape(2 * MESH, -1)


def whole_kernel(
    parts_y, parts_z,
    cells, fractions, charges, influence, shells, tx_hbm, wy_hbm, wz_hbm,
    out, joined,
    xs_all, xst_all, ys_all, zw_all, zc_all, xst, ys, zw, zc, table, acc, halo_y, edge, halo_z, wave, arrived, made, landed,
    tx, wy, wz, weights, labels_in, total, bins, pack_own, pack_z, pack_sum, pack_x, staged,
    load, send_hy, take_hy, send_hz, take_hz, send_x, take_x, send_z, take_z, store,
    send_rz, take_rz, send_rx, take_rx,
):
    ny = MESH // parts_y
    nz = MESH // parts_z
    nkx = MESH // parts_y
    nky = MESH // parts_z
    ext_y = ny + HALO_Y
    chunks = nz // PLANES
    turns = nkx // GROUP
    ahead = [AHEAD[4 * t // turns] for t in range(turns)]
    atoms = charges.shape[1]
    me_x = lax.axis_index("gx")
    me_z = lax.axis_index("gy")
    mesh_id = pl.DeviceIdType.MESH

    loads = [
        pltpu.make_async_copy(tx_hbm, tx, load.at[0]),
        pltpu.make_async_copy(wy_hbm, wy, load.at[1]),
        pltpu.make_async_copy(wz_hbm, wz, load.at[2]),
        pltpu.make_async_copy(influence, weights, load.at[3]),
        pltpu.make_async_copy(shells, labels_in, load.at[4]),
    ]
    for item in loads:
        item.start()

    barrier = pltpu.get_barrier_semaphore()

    @pl.loop(1, parts_y)
    def _(offset):
        pl.semaphore_signal(
            barrier, inc=1, device_id=(lax.rem(me_x + offset, parts_y), me_z), device_id_type=mesh_id
        )

    @pl.loop(1, parts_z)
    def _(offset):
        pl.semaphore_signal(
            barrier, inc=1, device_id=(me_x, lax.rem(me_z + offset, parts_z)), device_id_type=mesh_id
        )

    def remote(source, target, send, receive, device):
        return pltpu.make_async_remote_copy(
            src_ref=source,
            dst_ref=target,
            send_sem=send,
            recv_sem=receive,
            device_id=device,
            device_id_type=mesh_id,
        )

    next_x = lax.rem(me_x + 1, parts_y)
    next_z = lax.rem(me_z + 1, parts_z)

    def copy_hy(turn):
        return remote(
            acc.at[turn, :, pl.ds(ny * PLANES, HALO_Y * PLANES)],
            halo_y.at[turn],
            send_hy,
            take_hy.at[turn],
            (next_x, me_z),
        )

    def copy_hz():
        return remote(edge, halo_z, send_hz, take_hz, (me_x, next_z))

    def copy_x(chunk, source, target):
        return remote(
            wave.at[chunk, target],
            arrived.at[chunk, source],
            send_x,
            take_x.at[chunk],
            (source + target - me_x, me_z),
        )

    def copy_z(chunk, part, source, target):
        return remote(
            made.at[chunk, target, part],
            landed.at[chunk, source, part],
            send_z,
            take_z.at[part],
            (me_x, source + target - me_z),
        )

    start_y = me_x * ny
    start_z = me_z * nz

    def prepare(block, lanes):
        xs, xst_own, ys_own, zw_own, zc_own = (
            xs_all.at[block],
            xst_all.at[block],
            ys_all.at[block],
            zw_all.at[block],
            zc_all.at[block],
        )
        splines = spline(fractions[:, lanes])
        charge = charges[0:1, lanes]
        value, place = tiles_of(
            cells[0:1, lanes], [w[0:1] * charge for w in splines], 16, jnp.bfloat16
        )
        place = (place & (MESH // 16 - 1)).astype(jnp.float32).astype(jnp.bfloat16)
        none = jnp.zeros_like(value)
        for tile in range(MESH // 16):
            xs[tile * 16 : tile * 16 + 16, :] = jnp.where(
                place == jnp.bfloat16(tile), value, none
            )
        turned = xs[...].T
        xst_own[...] = turned
        xst[lanes, :] = turned
        value, place = tiles_of(
            cells[1:2, lanes] - start_y, [w[1:2] for w in splines], 8, jnp.float32
        )
        for tile in range(ys.shape[0] // 8):
            rows = jnp.where(place == tile, value, 0.0)
            ys_own[tile * 8 : tile * 8 + 8, :] = rows
            ys[tile * 8 : tile * 8 + 8, lanes] = rows
        for offset in range(4):
            zw_own[offset : offset + 1, :] = splines[offset][2:3]
            zw[offset : offset + 1, lanes] = splines[offset][2:3]
        spot = cells[2:3, lanes] - start_z
        zc_own[...] = spot
        zc[0:1, lanes] = spot
        return (xst_own, ys_own, zw_own, zc_own), slice(0, BLOCK)


    halo_turn = min(4, chunks - 1)

    def chunk_of(turn):
        later = jnp.where(turn == halo_turn, chunks, jnp.where(turn == chunks, 0, turn))
        return jnp.where(turn < halo_turn, turn + 1, later)

    steps = atoms // (BLOCK * SUBS)

    def spread_block(refs, lanes, base, buffer):
        xst, ys, zw, zc = refs
        shift = lax.broadcasted_iota(jnp.int32, (8, BLOCK), 0) - (zc[0:1, lanes] - base)
        zt = jnp.zeros((8, BLOCK), jnp.float32)
        for offset in range(4):
            zt = jnp.where(shift == offset, zw[offset : offset + 1, lanes], zt)
        for y in range(0, ext_y, 2):
            both = jnp.concatenate(
                [zt * ys[y : y + 1, lanes], zt * ys[y + 1 : y + 2, lanes]], axis=0
            )
            buffer[y * 8 : (y + 2) * 8, :] = both.astype(jnp.bfloat16)
        return dot(buffer[...], xst[lanes, :], NN)

    def spread_steps(turn, first, last, subs, fresh):
        base = chunk_of(turn) * PLANES

        @pl.loop(first, last)
        def _(block):
            sums = None
            for sub in range(subs):
                lanes = pl.ds(pl.multiple_of((block * subs + sub) * BLOCK, BLOCK), BLOCK)
                refs = (xst, ys, zw, zc)
                if fresh:
                    refs, lanes = prepare(sub, lanes)
                part = spread_block(refs, lanes, base, table.at[sub % BUFFERS])
                sums = part if sums is None else sums + part
            for half in range(2):
                acc[turn, half] += sums[:, half * 128 : (half + 1) * 128]

    def clear(turn):
        acc[turn] = jnp.zeros(acc.shape[1:], jnp.float32)

    @jax.named_scope("spread")
    def spread(turn, first, last):
        spread_steps(turn, first, last, SUBS, False)

    with jax.named_scope("first"):
        clear(0)
        spread_steps(0, 0, atoms // (BLOCK * FIRST_SUBS), FIRST_SUBS, True)
    with jax.named_scope("wait_barrier"):
        pl.semaphore_wait(barrier, parts_y + parts_z - 2)
        for item in loads:
            item.wait()
    copy_hy(0).start()

    @jax.named_scope("stage_x")
    def stage_x(turn):
        with jax.named_scope("wait_hy"):
            copy_hy(turn).wait_recv()
        acc[turn, :, 0 : HALO_Y * PLANES, :] += halo_y[turn]

        @pl.when(turn == halo_turn)
        def _():
            for z in range(HALO_Z):
                for half in range(2):
                    edge[half, z * ny : (z + 1) * ny, :] = acc[
                        turn, half, pl.ds(z, ny, stride=PLANES), :
                    ]
            copy_hz().start()

        @pl.when(turn == chunks)
        def _():
            copy_hz().wait_recv()
            for z in range(HALO_Z):
                for half in range(2):
                    acc[turn, half, pl.ds(z, ny, stride=PLANES), :] += halo_z[
                        half, z * ny : (z + 1) * ny, :
                    ]

        @pl.when(turn != halo_turn)
        def _():
            chunk = chunk_of(turn)
            values = jnp.concatenate(
                [
                    jnp.concatenate(
                        [acc[turn, half, pl.ds(z, ny, stride=PLANES), :] for half in range(2)],
                        axis=1,
                    )
                    for z in range(PLANES)
                ],
                axis=0,
            )
            result = dot3((tx[0], tx[1]), split(values), NT)
            lanes = PLANES * ny
            wave[chunk, :, 0:nkx, :] = result[:MESH].reshape(parts_y, nkx, lanes)
            wave[chunk, :, nkx : 2 * nkx, :] = result[MESH:].reshape(parts_y, nkx, lanes)

            @pl.loop(1, parts_y)
            def _(offset):
                copy_x(chunk, me_x, lax.rem(me_x + offset, parts_y)).start()

            arrived[chunk, me_x] = wave[chunk, me_x]

    def send_part(chunk, part):
        half = parts_z // 2
        mine, spot = me_z // half, me_z % half

        @pl.loop(0, half)
        def _(offset):
            copy_z(chunk, part, me_z, (1 - mine) * half + (spot + offset) % half).start()

        @pl.loop(1, half)
        def _(offset):
            copy_z(chunk, part, me_z, mine * half + (spot + offset) % half).start()

    @jax.named_scope("wait_x")
    def wait_x(chunk):
        span = arrived.at[chunk, pl.ds(0, parts_y - 1)]
        pltpu.make_async_copy(span, span, take_x.at[chunk]).wait()

    @jax.named_scope("stage_y")
    def stage_y(turn):
        chunk = chunk_of(turn)
        wait_x(chunk)

        rows = []
        for z in range(PLANES):
            lanes = slice(z * ny, (z + 1) * ny)
            both = [
                arrived[chunk, s, part * nkx : (part + 1) * nkx, lanes]
                for part in range(2)
                for s in range(parts_y)
            ]
            rows.append(jnp.concatenate(both, axis=1))
        values = split(jnp.concatenate(rows, axis=0))
        result = dot3(values, (wy[0], wy[1]), NN)
        width = made.shape[4]
        for q in range(parts_z):
            lanes = slice(q * width, (q + 1) * width)
            for t in range(turns):
                for z in range(PLANES):
                    row = z * nkx + t * GROUP
                    made[chunk, q, t, z * GROUP : (z + 1) * GROUP, :] = result[
                        row : row + GROUP, lanes
                    ]
        for t in range(turns):

            @pl.when(turn < ahead[t])
            def _():
                send_part(chunk, t)

        landed[chunk, me_z] = made[chunk, me_z]

    @pl.loop(1, chunks + 3)
    def _(turn):
        @pl.when(turn <= chunks)
        def _():
            clear(turn)
            spread(turn, 0, steps // 2)

        @pl.when(turn <= chunks + 1)
        def _():
            stage_x(turn - 1)

        @pl.when(jnp.logical_and(turn >= 2, turn != halo_turn + 2))
        def _():
            stage_y(turn - 2)

        @pl.when(turn <= chunks)
        def _():
            spread(turn, steps // 2, steps)
            copy_hy(turn).start()

    for t in range(turns):

        @pl.loop(min(ahead[t], chunks + 1), chunks + 1)
        def _(turn):
            @pl.when(turn != halo_turn)
            def _():
                send_part(chunk_of(turn), t)

    total[...] = jnp.zeros_like(total)
    bins[...] = jnp.zeros_like(bins)
    wave_y = wave_numbers(me_z * nky + lax.broadcasted_iota(jnp.int32, (nky, MESH), 0))
    wave_z = wave_numbers(lax.broadcasted_iota(jnp.int32, (nky, MESH), 1))

    @jax.named_scope("wait_z")
    def take_part(part):
        span = landed.at[:, pl.ds(0, parts_z - 1), 0]
        pltpu.make_async_copy(span, span, take_z.at[part]).wait()

    @jax.named_scope("final")
    def final(t):
        plane = wave_y * wave_y + wave_z * wave_z
        labels = lax.broadcasted_iota(jnp.int32, (16, MESH), 0)

        @pl.loop(0, GROUP // 2)
        def _(pair):
            turned = []
            for k in range(2):
                cube = jnp.concatenate(
                    [
                        landed[chunk, q, t, pl.ds(pair * 2 + k, PLANES, stride=GROUP), :]
                        for q in range(parts_z)
                        for chunk in range(chunks)
                    ],
                    axis=0,
                )
                turned.append(cube.T[: 2 * nky])
            result = dot3(split(jnp.concatenate(turned, axis=0)), (wz[0], wz[1]), NN)
            for k in range(2):
                first = result[2 * k * nky : (2 * k + 1) * nky]
                second = result[(2 * k + 1) * nky : (2 * k + 2) * nky]
                real = first[:, :MESH] + second[:, MESH:]
                imag = second[:, :MESH] - first[:, MESH:]
                index = t * GROUP + pair * 2 + k
                number = me_x * nkx + index
                wave_x = jnp.where(number < MESH // 2, number, number - MESH).astype(jnp.float32)
                squared = plane + wave_x * wave_x
                keep = jnp.where(squared > 0.0, 1.0, 0.0)
                weight = keep * weights[index]
                staged[0, index] = weight * real
                staged[1, index] = weight * imag
                power = real * real + imag * imag
                weighted = weight * power
                coef = weighted * (
                    2.0 * (1.0 + squared * (1.0 / SCREEN)) / (squared + 1.0 - keep)
                )
                total[0] += weighted
                total[1] += coef
                total[2] += coef * wave_x
                total[3] += coef * (wave_x * wave_x)
                shell = labels_in[index]
                upper = shell >> 4
                lower = shell & 15
                sums = None
                for group in range(nky // 16):
                    left = []
                    right = []
                    for row in range(group * 16, group * 16 + 16):
                        left.append(
                            jnp.where(
                                upper[row : row + 1] == labels, power[row : row + 1], 0.0
                            ).astype(jnp.bfloat16)
                        )
                        right.append(
                            jnp.where(lower[row : row + 1] == labels, 1.0, 0.0).astype(
                                jnp.bfloat16
                            )
                        )
                    part = dot(
                        jnp.concatenate(left, axis=0), jnp.concatenate(right, axis=0), NT
                    )
                    sums = part if sums is None else sums + part
                bins[...] += sums

    @pl.loop(0, turns)
    def _(t):
        take_part(t)
        final(t)
        rows = pl.ds(t * GROUP, GROUP)
        pltpu.make_async_copy(staged.at[:, rows], out.at[:, rows], store).start()

    one = total[1]
    over_x = total[2]
    parts = [
        total[0],
        total[3],
        over_x * wave_y,
        over_x * wave_z,
        one * wave_y * wave_y,
        one * wave_y * wave_z,
        one * wave_z * wave_z,
        jnp.zeros_like(one),
    ]
    values = jnp.concatenate(
        [jnp.sum(p, axis=0, keepdims=True) for p in parts], axis=0
    )
    values = jnp.sum(values, axis=1, keepdims=True)
    row = lax.broadcasted_iota(jnp.int32, bins.shape, 0)
    lane = lax.broadcasted_iota(jnp.int32, bins.shape, 1)
    kept = jnp.where((row >> 4) == (lane >> 4), bins[...], 0.0)
    folded = jnp.sum(kept.reshape(16, 16, MESH), axis=0)
    select = jnp.where((row & 15) == (lane & 15), 1.0, 0.0)
    shell_sums = lax.dot_general(
        folded,
        select,
        NN,
        precision=lax.Precision.HIGHEST,
        preferred_element_type=jnp.float32,
    )
    shell_sums = jnp.where(row[:16] == (lane[:16] >> 4), shell_sums, 0.0)
    shell_sums = jnp.sum(shell_sums, axis=0, keepdims=True)
    slot = lax.broadcasted_iota(jnp.int32, (8, 128), 0)
    sums = jnp.where(slot == 0, shell_sums[:, :128], shell_sums[:, 128:])
    mine = jnp.concatenate([jnp.broadcast_to(values, (8, 128)), sums], axis=0)

    def copy_rz(source, target):
        return remote(
            pack_own, pack_z.at[source], send_rz, take_rz,
            (me_x, source + target - me_z),
        )

    def copy_rx(source, target):
        return remote(
            pack_sum, pack_x.at[source], send_rx, take_rx,
            (source + target - me_x, me_z),
        )

    pack_own[...] = mine
    pack_z[me_z] = mine

    @pl.loop(1, parts_z)
    def _(offset):
        copy_rz(me_z, lax.rem(me_z + offset, parts_z)).start()

    def wait_all(group, count, semaphore):
        span = group.at[pl.ds(0, count)]
        pltpu.make_async_copy(span, span, semaphore).wait()

    with jax.named_scope("wait_rz"):
        wait_all(pack_z, parts_z - 1, take_rz)

    value = pack_z[0]
    for q in range(1, parts_z):
        value = value + pack_z[q]
    pack_sum[...] = value
    pack_x[me_x] = value

    @pl.loop(1, parts_y)
    def _(offset):
        copy_rx(me_x, lax.rem(me_x + offset, parts_y)).start()

    pltpu.make_async_copy(staged, out, store).wait()
    span = halo_y.at[:]
    pltpu.make_async_copy(span, span, send_hy).wait()
    copy_hz().wait_send()
    span = wave.at[:, pl.ds(0, parts_y - 1)]
    pltpu.make_async_copy(span, span, send_x).wait()
    span = made.at[:, pl.ds(0, parts_z - 1)]
    pltpu.make_async_copy(span, span, send_z).wait()

    with jax.named_scope("wait_rx"):
        wait_all(pack_x, parts_y - 1, take_rx)

    value = pack_x[0]
    for p in range(1, parts_y):
        value = value + pack_x[p]
    joined[...] = value

    wait_all(pack_z, parts_z - 1, send_rz)
    wait_all(pack_x, parts_y - 1, send_rx)


def whole(cells, fractions, charges, influence, shells, parts_y, parts_z):
    atoms = charges.shape[1]
    ny = MESH // parts_y
    nz = MESH // parts_z
    nkx = MESH // parts_y
    nky = MESH // parts_z
    ext_y = ny + HALO_Y
    chunks = nz // PLANES
    turns = nkx // GROUP
    cosine, sine, along_x = tables()
    tx = jnp.stack(table_pair(along_x))
    wy = jnp.stack(table_pair(table_y(cosine, sine, parts_z)))
    wz = jnp.stack(table_pair(np.concatenate([cosine, sine], axis=1)))
    f32, bf16 = jnp.float32, jnp.bfloat16
    vmem = pltpu.VMEM
    dma = lambda *shape: pltpu.SemaphoreType.DMA(shape)
    return pl.pallas_call(
        functools.partial(whole_kernel, parts_y, parts_z),
        in_specs=[pl.BlockSpec(memory_space=pltpu.VMEM)] * 3
        + [pl.BlockSpec(memory_space=pl.ANY)] * 5,
        out_specs=[
            pl.BlockSpec(memory_space=pl.ANY),
            pl.BlockSpec(memory_space=pltpu.VMEM),
        ],
        out_shape=[
            jax.ShapeDtypeStruct((2,) + influence.shape, f32),
            jax.ShapeDtypeStruct((PACK, 128), f32),
        ],
        scratch_shapes=[
            vmem((FIRST_SUBS, MESH, BLOCK), bf16),
            vmem((FIRST_SUBS, BLOCK, MESH), bf16),
            vmem((FIRST_SUBS, (ext_y + 7) // 8 * 8, BLOCK), f32),
            vmem((FIRST_SUBS, 4, BLOCK), f32),
            vmem((FIRST_SUBS, 1, BLOCK), jnp.int32),
            vmem((atoms, MESH), bf16),
            vmem(((ext_y + 7) // 8 * 8, atoms), f32),
            vmem((4, atoms), f32),
            vmem((1, atoms), jnp.int32),
            vmem((BUFFERS, ext_y * PLANES, BLOCK), bf16),
            vmem((chunks + 1, 2, ext_y * PLANES, MESH // 2), f32),
            vmem((chunks + 1, 2, HALO_Y * PLANES, MESH // 2), f32),
            vmem((2, HALO_Z * ny, MESH // 2), f32),
            vmem((2, HALO_Z * ny, MESH // 2), f32),
            vmem((chunks, parts_y, 2 * nkx, PLANES * ny), f32),
            vmem((chunks, parts_y, 2 * nkx, PLANES * ny), f32),
            vmem((chunks, parts_z, turns, PLANES * GROUP, max(2 * nky, 128)), f32),
            vmem((chunks, parts_z, turns, PLANES * GROUP, max(2 * nky, 128)), f32),
            vmem(tx.shape, bf16),
            vmem(wy.shape, bf16),
            vmem(wz.shape, bf16),
            vmem(influence.shape, f32),
            vmem(shells.shape, jnp.int32),
            vmem((4, nky, MESH), f32),
            vmem((MESH, MESH), f32),
            vmem((PACK, 128), f32),
            vmem((parts_z, PACK, 128), f32),
            vmem((PACK, 128), f32),
            vmem((parts_y, PACK, 128), f32),
            vmem((2,) + influence.shape, f32),
            dma(5),
            pltpu.SemaphoreType.DMA,
            dma(chunks + 1),
            pltpu.SemaphoreType.DMA,
            pltpu.SemaphoreType.DMA,
            pltpu.SemaphoreType.DMA,
            dma(chunks),
            pltpu.SemaphoreType.DMA,
            dma(turns),
            pltpu.SemaphoreType.DMA,
            pltpu.SemaphoreType.DMA,
            pltpu.SemaphoreType.DMA,
            pltpu.SemaphoreType.DMA,
            pltpu.SemaphoreType.DMA,
        ],
        compiler_params=pltpu.CompilerParams(
            collective_id=0, has_side_effects=True, vmem_limit_bytes=58 << 20
        ),
        name="whole",
    )(cells, fractions, charges, influence, shells, tx, wy, wz)


def finish_kernel(hat, joined, out, energy, virial, spectrum, moved, take, give):
    count = moved.shape[1]
    step = hat.shape[1] // count
    spots = [(part, index) for part in range(2) for index in range(count)]

    def copy_in(part, index):
        rows = pl.ds(index * step, step)
        return pltpu.make_async_copy(
            hat.at[part, rows], moved.at[part, index], take.at[part, index]
        )

    def copy_out(part, index):
        rows = pl.ds(index * step, step)
        return pltpu.make_async_copy(
            moved.at[part, index], out.at[part, rows], give.at[part, index]
        )

    for spot in spots:
        copy_in(*spot).start()
    scale = 0.5 / MESH**3
    values = [joined[index : index + 1, 0:1] for index in range(7)]
    energy[...] = scale * values[0]
    row = lax.broadcasted_iota(jnp.int32, (3, 3), 0)
    column = lax.broadcasted_iota(jnp.int32, (3, 3), 1)
    result = jnp.where(row == column, values[0], 0.0)
    for spot, index in enumerate((1, 2, 3, 2, 4, 5, 3, 5, 6)):
        here = jnp.logical_and(row == spot // 3, column == spot % 3)
        result = result - jnp.where(here, values[index], 0.0)
    virial[...] = scale * result
    spectrum[...] = joined[8:10, :] * (SHELLS / MESH**3)
    for spot in spots:
        copy_in(*spot).wait()
        copy_out(*spot).start()
    for spot in spots:
        copy_out(*spot).wait()


def finish(hat, joined, count=4):
    step = hat.shape[1] // count
    f32 = jnp.float32
    return pl.pallas_call(
        finish_kernel,
        in_specs=[
            pl.BlockSpec(memory_space=pl.ANY),
            pl.BlockSpec(memory_space=pltpu.VMEM),
        ],
        out_specs=[pl.BlockSpec(memory_space=pl.ANY)]
        + [pl.BlockSpec(memory_space=pltpu.VMEM)] * 3,
        out_shape=[
            jax.ShapeDtypeStruct(hat.shape, f32),
            jax.ShapeDtypeStruct((1, 1), f32),
            jax.ShapeDtypeStruct((3, 3), f32),
            jax.ShapeDtypeStruct((2, 128), f32),
        ],
        scratch_shapes=[
            pltpu.VMEM((2, count, step) + hat.shape[2:], f32),
            pltpu.SemaphoreType.DMA((2, count)),
            pltpu.SemaphoreType.DMA((2, count)),
        ],
        compiler_params=pltpu.CompilerParams(vmem_limit_bytes=62 << 20),
        name="finish",
    )(hat, joined)


def shards(cells, fractions, charges, influence, shells):
    parts_y = lax.axis_size("gx")
    parts_z = lax.axis_size("gy")
    hat, joined = whole(cells, fractions, charges[None], influence, shells, parts_y, parts_z)
    potential_hat, energy, virial, spectrum = finish(hat, joined)
    return (potential_hat, energy.reshape(()), virial, spectrum.reshape(SHELLS))


def solution(mesh):
    return jax.shard_map(
        shards,
        mesh=mesh,
        in_specs=(
            P(None, ("gx", "gy")),
            P(None, ("gx", "gy")),
            P(("gx", "gy")),
            P("gx", "gy", None),
            P("gx", "gy", None),
        ),
        out_specs=(P(None, "gx", "gy", None), P(), P(), P()),
        check_vma=False,
    )
```

```python
import functools
import math

import jax
import jax.numpy as jnp
import numpy as np
from jax import lax
from jax.experimental import pallas as pl
from jax.experimental.pallas import tpu as pltpu
from jax.sharding import PartitionSpec as P

MESH = 256
SHELLS = 256
SCREEN = 4096
HALO_Y = 4
HALO_Z = 3
PLANES = 8
GROUP = 4
BLOCK = 1024
SUBS = 8
FIRST_SUBS = 8
BUFFERS = 4
PACK = 16
SIXTH = 1.0 / 6.0
AHEAD = (9, 9, 7, 1)
NT = (((1,), (1,)), ((), ()))
NN = (((1,), (0,)), ((), ()))


def spline(frac):
    cube = frac * frac * frac
    square = frac * frac
    rest = 1.0 - frac
    return (
        rest * rest * rest * SIXTH,
        (3.0 * cube - 6.0 * square + 4.0) * SIXTH,
        (-3.0 * cube + 3.0 * square + 3.0 * frac + 1.0) * SIXTH,
        cube * SIXTH,
    )


def split(values):
    high = values.astype(jnp.bfloat16)
    low = (values - high.astype(jnp.float32)).astype(jnp.bfloat16)
    return high, low


def dot(left, right, dims):
    return lax.dot_general(left, right, dims, preferred_element_type=jnp.float32)


def dot3(left, right, dims):
    return (
        dot(left[0], right[0], dims) + dot(left[0], right[1], dims) + dot(left[1], right[0], dims)
    )


def table_pair(table):
    high = jnp.asarray(table.astype(np.float32)).astype(jnp.bfloat16)
    low = jnp.asarray(
        (table - table.astype(np.float32).astype(jnp.bfloat16).astype(np.float64)).astype(np.float32)
    ).astype(jnp.bfloat16)
    return high, low


def wave_tables():
    index = np.arange(MESH)
    angle = (index[:, None] * index[None, :] % MESH) * (2.0 * math.pi / MESH)
    factor = 1.0 / math.sqrt(MESH)
    return np.cos(angle) * factor, np.sin(angle) * factor


def wave_numbers(index):
    return jnp.where(index < MESH // 2, index, index - MESH).astype(jnp.float32)


def tiles_of(cell, weights, rows, kind):
    shape = (rows, cell.shape[1])
    row = lax.broadcasted_iota(jnp.int32, shape, 0)
    low = cell & (rows - 1)
    shift = (row - low) & (rows - 1)
    value = jnp.zeros(shape, jnp.float32)
    for offset in range(4):
        value = jnp.where(shift == offset, weights[offset], value)
    tile = (cell // rows) + jnp.where(row < low, 1, 0)
    return value.astype(kind), tile


def tables():
    cosine, sine = wave_tables()
    along_x = np.concatenate([cosine, -sine], axis=0)
    return cosine, sine, along_x


def table_y(cosine, sine, parts_z):
    rows = MESH // parts_z
    table = np.zeros((2, MESH, parts_z, max(2 * rows, 128)))
    cosine = cosine.reshape(MESH, parts_z, rows)
    sine = sine.reshape(MESH, parts_z, rows)
    table[0, :, :, :rows] = cosine
    table[0, :, :, rows : 2 * rows] = -sine
    table[1, :, :, :rows] = sine
    table[1, :, :, rows : 2 * rows] = cosine
    return table.reshape(2 * MESH, -1)


def whole_kernel(
    parts_y, parts_z,
    cells, fractions, charges, influence, shells, tx_hbm, wy_hbm, wz_hbm,
    out, joined,
    xs_all, xst_all, ys_all, zw_all, zc_all, xst, ys, zw, zc, table, acc, halo_y, edge, halo_z, wave, arrived, made, landed,
    tx, wy, wz, weights, labels_in, total, bins, pack_own, pack_z, pack_sum, pack_x, staged,
    load, send_hy, take_hy, send_hz, take_hz, send_x, take_x, send_z, take_z, store,
    send_rz, take_rz, send_rx, take_rx,
):
    ny = MESH // parts_y
    nz = MESH // parts_z
    nkx = MESH // parts_y
    nky = MESH // parts_z
    ext_y = ny + HALO_Y
    chunks = nz // PLANES
    turns = nkx // GROUP
    ahead = [AHEAD[4 * t // turns] for t in range(turns)]
    atoms = charges.shape[1]
    me_x = lax.axis_index("gx")
    me_z = lax.axis_index("gy")
    mesh_id = pl.DeviceIdType.MESH

    loads = [
        pltpu.make_async_copy(tx_hbm, tx, load.at[0]),
        pltpu.make_async_copy(wy_hbm, wy, load.at[1]),
        pltpu.make_async_copy(wz_hbm, wz, load.at[2]),
        pltpu.make_async_copy(influence, weights, load.at[3]),
        pltpu.make_async_copy(shells, labels_in, load.at[4]),
    ]
    for item in loads:
        item.start()

    barrier = pltpu.get_barrier_semaphore()

    @pl.loop(1, parts_y)
    def _(offset):
        pl.semaphore_signal(
            barrier, inc=1, device_id=(lax.rem(me_x + offset, parts_y), me_z), device_id_type=mesh_id
        )

    @pl.loop(1, parts_z)
    def _(offset):
        pl.semaphore_signal(
            barrier, inc=1, device_id=(me_x, lax.rem(me_z + offset, parts_z)), device_id_type=mesh_id
        )

    def remote(source, target, send, receive, device):
        return pltpu.make_async_remote_copy(
            src_ref=source,
            dst_ref=target,
            send_sem=send,
            recv_sem=receive,
            device_id=device,
            device_id_type=mesh_id,
        )

    next_x = lax.rem(me_x + 1, parts_y)
    next_z = lax.rem(me_z + 1, parts_z)

    def copy_hy(turn):
        return remote(
            acc.at[turn, :, pl.ds(ny * PLANES, HALO_Y * PLANES)],
            halo_y.at[turn],
            send_hy,
            take_hy.at[turn],
            (next_x, me_z),
        )

    def copy_hz():
        return remote(edge, halo_z, send_hz, take_hz, (me_x, next_z))

    def copy_x(chunk, source, target):
        return remote(
            wave.at[chunk, target],
            arrived.at[chunk, source],
            send_x,
            take_x.at[chunk],
            (source + target - me_x, me_z),
        )

    def copy_z(chunk, part, source, target):
        return remote(
            made.at[chunk, target, part],
            landed.at[chunk, source, part],
            send_z,
            take_z.at[part],
            (me_x, source + target - me_z),
        )

    start_y = me_x * ny
    start_z = me_z * nz

    def prepare(block, lanes):
        xs, xst_own, ys_own, zw_own, zc_own = (
            xs_all.at[block % BUFFERS],
            xst_all.at[block % BUFFERS],
            ys_all.at[block % BUFFERS],
            zw_all.at[block % BUFFERS],
            zc_all.at[block % BUFFERS],
        )
        splines = spline(fractions[:, lanes])
        charge = charges[0:1, lanes]
        value, place = tiles_of(
            cells[0:1, lanes], [w[0:1] * charge for w in splines], 16, jnp.bfloat16
        )
        place = (place & (MESH // 16 - 1)).astype(jnp.float32).astype(jnp.bfloat16)
        none = jnp.zeros_like(value)
        for tile in range(MESH // 16):
            xs[tile * 16 : tile * 16 + 16, :] = jnp.where(
                place == jnp.bfloat16(tile), value, none
            )
        turned = xs[...].T
        xst_own[...] = turned
        xst[lanes, :] = turned
        value, place = tiles_of(
            cells[1:2, lanes] - start_y, [w[1:2] for w in splines], 8, jnp.float32
        )
        for tile in range(ys.shape[0] // 8):
            rows = jnp.where(place == tile, value, 0.0)
            ys_own[tile * 8 : tile * 8 + 8, :] = rows
            ys[tile * 8 : tile * 8 + 8, lanes] = rows
        for offset in range(4):
            zw_own[offset : offset + 1, :] = splines[offset][2:3]
            zw[offset : offset + 1, lanes] = splines[offset][2:3]
        spot = cells[2:3, lanes] - start_z
        zc_own[...] = spot
        zc[0:1, lanes] = spot
        return (xst_own, ys_own, zw_own, zc_own), slice(0, BLOCK)


    halo_turn = min(4, chunks - 1)

    def chunk_of(turn):
        later = jnp.where(turn == halo_turn, chunks, jnp.where(turn == chunks, 0, turn))
        return jnp.where(turn < halo_turn, turn + 1, later)

    steps = atoms // (BLOCK * SUBS)

    def spread_block(refs, lanes, base, buffer):
        xst, ys, zw, zc = refs
        shift = lax.broadcasted_iota(jnp.int32, (8, BLOCK), 0) - (zc[0:1, lanes] - base)
        zt = jnp.zeros((8, BLOCK), jnp.float32)
        for offset in range(4):
            zt = jnp.where(shift == offset, zw[offset : offset + 1, lanes], zt)
        for y in range(0, ext_y, 2):
            both = jnp.concatenate(
                [zt * ys[y : y + 1, lanes], zt * ys[y + 1 : y + 2, lanes]], axis=0
            )
            buffer[y * 8 : (y + 2) * 8, :] = both.astype(jnp.bfloat16)
        return dot(buffer[...], xst[lanes, :], NN)

    def spread_steps(turn, first, last, subs, fresh):
        base = chunk_of(turn) * PLANES

        @pl.loop(first, last)
        def _(block):
            sums = None
            for sub in range(subs):
                lanes = pl.ds(pl.multiple_of((block * subs + sub) * BLOCK, BLOCK), BLOCK)
                refs = (xst, ys, zw, zc)
                if fresh:
                    refs, lanes = prepare(sub, lanes)
                part = spread_block(refs, lanes, base, table.at[sub % BUFFERS])
                sums = part if sums is None else sums + part
            for half in range(2):
                acc[turn, half] += sums[:, half * 128 : (half + 1) * 128]

    def clear(turn):
        acc[turn] = jnp.zeros(acc.shape[1:], jnp.float32)

    @jax.named_scope("spread")
    def spread(turn, first, last):
        spread_steps(turn, first, last, SUBS, False)

    with jax.named_scope("first"):
        clear(0)
        spread_steps(0, 0, atoms // (BLOCK * FIRST_SUBS), FIRST_SUBS, True)
    with jax.named_scope("wait_barrier"):
        pl.semaphore_wait(barrier, parts_y + parts_z - 2)
        for item in loads:
            item.wait()
    copy_hy(0).start()

    @jax.named_scope("stage_x")
    def stage_x(turn):
        with jax.named_scope("wait_hy"):
            copy_hy(turn).wait_recv()
        acc[turn, :, 0 : HALO_Y * PLANES, :] += halo_y[turn]

        @pl.when(turn == halo_turn)
        def _():
            for z in range(HALO_Z):
                for half in range(2):
                    edge[half, z * ny : (z + 1) * ny, :] = acc[
                        turn, half, pl.ds(z, ny, stride=PLANES), :
                    ]
            copy_hz().start()

        @pl.when(turn == chunks)
        def _():
            copy_hz().wait_recv()
            for z in range(HALO_Z):
                for half in range(2):
                    acc[turn, half, pl.ds(z, ny, stride=PLANES), :] += halo_z[
                        half, z * ny : (z + 1) * ny, :
                    ]

        @pl.when(turn != halo_turn)
        def _():
            chunk = chunk_of(turn)
            values = jnp.concatenate(
                [
                    jnp.concatenate(
                        [acc[turn, half, pl.ds(z, ny, stride=PLANES), :] for half in range(2)],
                        axis=1,
                    )
                    for z in range(PLANES)
                ],
                axis=0,
            )
            result = dot3((tx[0], tx[1]), split(values), NT)
            lanes = PLANES * ny
            wave[chunk, :, 0:nkx, :] = result[:MESH].reshape(parts_y, nkx, lanes)
            wave[chunk, :, nkx : 2 * nkx, :] = result[MESH:].reshape(parts_y, nkx, lanes)

            @pl.loop(1, parts_y)
            def _(offset):
                copy_x(chunk, me_x, lax.rem(me_x + offset, parts_y)).start()

            arrived[chunk, me_x] = wave[chunk, me_x]

    def send_part(chunk, part):
        half = parts_z // 2
        mine, spot = me_z // half, me_z % half

        @pl.loop(0, half)
        def _(offset):
            copy_z(chunk, part, me_z, (1 - mine) * half + (spot + offset) % half).start()

        @pl.loop(1, half)
        def _(offset):
            copy_z(chunk, part, me_z, mine * half + (spot + offset) % half).start()

    @jax.named_scope("wait_x")
    def wait_x(chunk):
        span = arrived.at[chunk, pl.ds(0, parts_y - 1)]
        pltpu.make_async_copy(span, span, take_x.at[chunk]).wait()

    @jax.named_scope("stage_y")
    def stage_y(turn):
        chunk = chunk_of(turn)
        wait_x(chunk)

        rows = []
        for z in range(PLANES):
            lanes = slice(z * ny, (z + 1) * ny)
            both = [
                arrived[chunk, s, part * nkx : (part + 1) * nkx, lanes]
                for part in range(2)
                for s in range(parts_y)
            ]
            rows.append(jnp.concatenate(both, axis=1))
        values = split(jnp.concatenate(rows, axis=0))
        result = dot3(values, (wy[0], wy[1]), NN)
        width = made.shape[4]
        for q in range(parts_z):
            lanes = slice(q * width, (q + 1) * width)
            for t in range(turns):
                for z in range(PLANES):
                    row = z * nkx + t * GROUP
                    made[chunk, q, t, z * GROUP : (z + 1) * GROUP, :] = result[
                        row : row + GROUP, lanes
                    ]
        for t in range(turns):

            @pl.when(turn < ahead[t])
            def _():
                send_part(chunk, t)

        landed[chunk, me_z] = made[chunk, me_z]

    @pl.loop(1, chunks + 3)
    def _(turn):
        @pl.when(turn <= chunks)
        def _():
            clear(turn)
            spread(turn, 0, steps // 2)

        @pl.when(turn <= chunks + 1)
        def _():
            stage_x(turn - 1)

        @pl.when(jnp.logical_and(turn >= 2, turn != halo_turn + 2))
        def _():
            stage_y(turn - 2)

        @pl.when(turn <= chunks)
        def _():
            spread(turn, steps // 2, steps)
            copy_hy(turn).start()

    for t in range(turns):

        @pl.loop(min(ahead[t], chunks + 1), chunks + 1)
        def _(turn):
            @pl.when(turn != halo_turn)
            def _():
                send_part(chunk_of(turn), t)

    total[...] = jnp.zeros_like(total)
    bins[...] = jnp.zeros_like(bins)
    wave_y = wave_numbers(me_z * nky + lax.broadcasted_iota(jnp.int32, (nky, MESH), 0))
    wave_z = wave_numbers(lax.broadcasted_iota(jnp.int32, (nky, MESH), 1))

    @jax.named_scope("wait_z")
    def take_part(part):
        span = landed.at[:, pl.ds(0, parts_z - 1), 0]
        pltpu.make_async_copy(span, span, take_z.at[part]).wait()

    @jax.named_scope("final")
    def final(t):
        plane = wave_y * wave_y + wave_z * wave_z
        labels = lax.broadcasted_iota(jnp.int32, (16, MESH), 0)

        @pl.loop(0, GROUP // 2)
        def _(pair):
            turned = []
            for k in range(2):
                cube = jnp.concatenate(
                    [
                        landed[chunk, q, t, pl.ds(pair * 2 + k, PLANES, stride=GROUP), :]
                        for q in range(parts_z)
                        for chunk in range(chunks)
                    ],
                    axis=0,
                )
                turned.append(cube.T[: 2 * nky])
            result = dot3(split(jnp.concatenate(turned, axis=0)), (wz[0], wz[1]), NN)
            for k in range(2):
                first = result[2 * k * nky : (2 * k + 1) * nky]
                second = result[(2 * k + 1) * nky : (2 * k + 2) * nky]
                real = first[:, :MESH] + second[:, MESH:]
                imag = second[:, :MESH] - first[:, MESH:]
                index = t * GROUP + pair * 2 + k
                number = me_x * nkx + index
                wave_x = jnp.where(number < MESH // 2, number, number - MESH).astype(jnp.float32)
                squared = plane + wave_x * wave_x
                keep = jnp.where(squared > 0.0, 1.0, 0.0)
                weight = keep * weights[index]
                staged[0, index] = weight * real
                staged[1, index] = weight * imag
                power = real * real + imag * imag
                weighted = weight * power
                coef = weighted * (
                    2.0 * (1.0 + squared * (1.0 / SCREEN)) / (squared + 1.0 - keep)
                )
                total[0] += weighted
                total[1] += coef
                total[2] += coef * wave_x
                total[3] += coef * (wave_x * wave_x)
                shell = labels_in[index]
                upper = shell >> 4
                lower = shell & 15
                sums = None
                for group in range(nky // 16):
                    left = []
                    right = []
                    for row in range(group * 16, group * 16 + 16):
                        left.append(
                            jnp.where(
                                upper[row : row + 1] == labels, power[row : row + 1], 0.0
                            ).astype(jnp.bfloat16)
                        )
                        right.append(
                            jnp.where(lower[row : row + 1] == labels, 1.0, 0.0).astype(
                                jnp.bfloat16
                            )
                        )
                    part = dot(
                        jnp.concatenate(left, axis=0), jnp.concatenate(right, axis=0), NT
                    )
                    sums = part if sums is None else sums + part
                bins[...] += sums

    @pl.loop(0, turns)
    def _(t):
        take_part(t)
        final(t)
        rows = pl.ds(t * GROUP, GROUP)
        pltpu.make_async_copy(staged.at[:, rows], out.at[:, rows], store).start()

    one = total[1]
    over_x = total[2]
    parts = [
        total[0],
        total[3],
        over_x * wave_y,
        over_x * wave_z,
        one * wave_y * wave_y,
        one * wave_y * wave_z,
        one * wave_z * wave_z,
        jnp.zeros_like(one),
    ]
    values = jnp.concatenate(
        [jnp.sum(p, axis=0, keepdims=True) for p in parts], axis=0
    )
    values = jnp.sum(values, axis=1, keepdims=True)
    row = lax.broadcasted_iota(jnp.int32, bins.shape, 0)
    lane = lax.broadcasted_iota(jnp.int32, bins.shape, 1)
    kept = jnp.where((row >> 4) == (lane >> 4), bins[...], 0.0)
    folded = jnp.sum(kept.reshape(16, 16, MESH), axis=0)
    select = jnp.where((row & 15) == (lane & 15), 1.0, 0.0)
    shell_sums = lax.dot_general(
        folded,
        select,
        NN,
        precision=lax.Precision.HIGHEST,
        preferred_element_type=jnp.float32,
    )
    shell_sums = jnp.where(row[:16] == (lane[:16] >> 4), shell_sums, 0.0)
    shell_sums = jnp.sum(shell_sums, axis=0, keepdims=True)
    slot = lax.broadcasted_iota(jnp.int32, (8, 128), 0)
    sums = jnp.where(slot == 0, shell_sums[:, :128], shell_sums[:, 128:])
    mine = jnp.concatenate([jnp.broadcast_to(values, (8, 128)), sums], axis=0)

    def copy_rz(source, target):
        return remote(
            pack_own, pack_z.at[source], send_rz, take_rz,
            (me_x, source + target - me_z),
        )

    def copy_rx(source, target):
        return remote(
            pack_sum, pack_x.at[source], send_rx, take_rx,
            (source + target - me_x, me_z),
        )

    pack_own[...] = mine
    pack_z[me_z] = mine

    @pl.loop(1, parts_z)
    def _(offset):
        copy_rz(me_z, lax.rem(me_z + offset, parts_z)).start()

    def wait_all(group, count, semaphore):
        span = group.at[pl.ds(0, count)]
        pltpu.make_async_copy(span, span, semaphore).wait()

    with jax.named_scope("wait_rz"):
        wait_all(pack_z, parts_z - 1, take_rz)

    value = pack_z[0]
    for q in range(1, parts_z):
        value = value + pack_z[q]
    pack_sum[...] = value
    pack_x[me_x] = value

    @pl.loop(1, parts_y)
    def _(offset):
        copy_rx(me_x, lax.rem(me_x + offset, parts_y)).start()

    pltpu.make_async_copy(staged, out, store).wait()
    span = halo_y.at[:]
    pltpu.make_async_copy(span, span, send_hy).wait()
    copy_hz().wait_send()
    span = wave.at[:, pl.ds(0, parts_y - 1)]
    pltpu.make_async_copy(span, span, send_x).wait()
    span = made.at[:, pl.ds(0, parts_z - 1)]
    pltpu.make_async_copy(span, span, send_z).wait()

    with jax.named_scope("wait_rx"):
        wait_all(pack_x, parts_y - 1, take_rx)

    value = pack_x[0]
    for p in range(1, parts_y):
        value = value + pack_x[p]
    joined[...] = value

    wait_all(pack_z, parts_z - 1, send_rz)
    wait_all(pack_x, parts_y - 1, send_rx)


def whole(cells, fractions, charges, influence, shells, parts_y, parts_z):
    atoms = charges.shape[1]
    ny = MESH // parts_y
    nz = MESH // parts_z
    nkx = MESH // parts_y
    nky = MESH // parts_z
    ext_y = ny + HALO_Y
    chunks = nz // PLANES
    turns = nkx // GROUP
    cosine, sine, along_x = tables()
    tx = jnp.stack(table_pair(along_x))
    wy = jnp.stack(table_pair(table_y(cosine, sine, parts_z)))
    wz = jnp.stack(table_pair(np.concatenate([cosine, sine], axis=1)))
    f32, bf16 = jnp.float32, jnp.bfloat16
    vmem = pltpu.VMEM
    dma = lambda *shape: pltpu.SemaphoreType.DMA(shape)
    return pl.pallas_call(
        functools.partial(whole_kernel, parts_y, parts_z),
        in_specs=[pl.BlockSpec(memory_space=pltpu.VMEM)] * 3
        + [pl.BlockSpec(memory_space=pl.ANY)] * 5,
        out_specs=[
            pl.BlockSpec(memory_space=pl.ANY),
            pl.BlockSpec(memory_space=pltpu.VMEM),
        ],
        out_shape=[
            jax.ShapeDtypeStruct((2,) + influence.shape, f32),
            jax.ShapeDtypeStruct((PACK, 128), f32),
        ],
        scratch_shapes=[
            vmem((BUFFERS, MESH, BLOCK), bf16),
            vmem((BUFFERS, BLOCK, MESH), bf16),
            vmem((BUFFERS, (ext_y + 7) // 8 * 8, BLOCK), f32),
            vmem((BUFFERS, 4, BLOCK), f32),
            vmem((BUFFERS, 1, BLOCK), jnp.int32),
            vmem((atoms, MESH), bf16),
            vmem(((ext_y + 7) // 8 * 8, atoms), f32),
            vmem((4, atoms), f32),
            vmem((1, atoms), jnp.int32),
            vmem((BUFFERS, ext_y * PLANES, BLOCK), bf16),
            vmem((chunks + 1, 2, ext_y * PLANES, MESH // 2), f32),
            vmem((chunks + 1, 2, HALO_Y * PLANES, MESH // 2), f32),
            vmem((2, HALO_Z * ny, MESH // 2), f32),
            vmem((2, HALO_Z * ny, MESH // 2), f32),
            vmem((chunks, parts_y, 2 * nkx, PLANES * ny), f32),
            vmem((chunks, parts_y, 2 * nkx, PLANES * ny), f32),
            vmem((chunks, parts_z, turns, PLANES * GROUP, max(2 * nky, 128)), f32),
            vmem((chunks, parts_z, turns, PLANES * GROUP, max(2 * nky, 128)), f32),
            vmem(tx.shape, bf16),
            vmem(wy.shape, bf16),
            vmem(wz.shape, bf16),
            vmem(influence.shape, f32),
            vmem(shells.shape, jnp.int32),
            vmem((4, nky, MESH), f32),
            vmem((MESH, MESH), f32),
            vmem((PACK, 128), f32),
            vmem((parts_z, PACK, 128), f32),
            vmem((PACK, 128), f32),
            vmem((parts_y, PACK, 128), f32),
            vmem((2,) + influence.shape, f32),
            dma(5),
            pltpu.SemaphoreType.DMA,
            dma(chunks + 1),
            pltpu.SemaphoreType.DMA,
            pltpu.SemaphoreType.DMA,
            pltpu.SemaphoreType.DMA,
            dma(chunks),
            pltpu.SemaphoreType.DMA,
            dma(turns),
            pltpu.SemaphoreType.DMA,
            pltpu.SemaphoreType.DMA,
            pltpu.SemaphoreType.DMA,
            pltpu.SemaphoreType.DMA,
            pltpu.SemaphoreType.DMA,
        ],
        compiler_params=pltpu.CompilerParams(
            collective_id=0, has_side_effects=True, vmem_limit_bytes=67043328
        ),
        name="whole",
    )(cells, fractions, charges, influence, shells, tx, wy, wz)


def finish_kernel(hat, joined, out, energy, virial, spectrum, moved, take, give):
    count = moved.shape[1]
    step = hat.shape[1] // count
    spots = [(part, index) for part in range(2) for index in range(count)]

    def copy_in(part, index):
        rows = pl.ds(index * step, step)
        return pltpu.make_async_copy(
            hat.at[part, rows], moved.at[part, index], take.at[part, index]
        )

    def copy_out(part, index):
        rows = pl.ds(index * step, step)
        return pltpu.make_async_copy(
            moved.at[part, index], out.at[part, rows], give.at[part, index]
        )

    for spot in spots:
        copy_in(*spot).start()
    scale = 0.5 / MESH**3
    values = [joined[index : index + 1, 0:1] for index in range(7)]
    energy[...] = scale * values[0]
    row = lax.broadcasted_iota(jnp.int32, (3, 3), 0)
    column = lax.broadcasted_iota(jnp.int32, (3, 3), 1)
    result = jnp.where(row == column, values[0], 0.0)
    for spot, index in enumerate((1, 2, 3, 2, 4, 5, 3, 5, 6)):
        here = jnp.logical_and(row == spot // 3, column == spot % 3)
        result = result - jnp.where(here, values[index], 0.0)
    virial[...] = scale * result
    spectrum[...] = joined[8:10, :] * (SHELLS / MESH**3)
    for spot in spots:
        copy_in(*spot).wait()
        copy_out(*spot).start()
    for spot in spots:
        copy_out(*spot).wait()


def finish(hat, joined, count=4):
    step = hat.shape[1] // count
    f32 = jnp.float32
    return pl.pallas_call(
        finish_kernel,
        in_specs=[
            pl.BlockSpec(memory_space=pl.ANY),
            pl.BlockSpec(memory_space=pltpu.VMEM),
        ],
        out_specs=[pl.BlockSpec(memory_space=pl.ANY)]
        + [pl.BlockSpec(memory_space=pltpu.VMEM)] * 3,
        out_shape=[
            jax.ShapeDtypeStruct(hat.shape, f32),
            jax.ShapeDtypeStruct((1, 1), f32),
            jax.ShapeDtypeStruct((3, 3), f32),
            jax.ShapeDtypeStruct((2, 128), f32),
        ],
        scratch_shapes=[
            pltpu.VMEM((2, count, step) + hat.shape[2:], f32),
            pltpu.SemaphoreType.DMA((2, count)),
            pltpu.SemaphoreType.DMA((2, count)),
        ],
        compiler_params=pltpu.CompilerParams(vmem_limit_bytes=62 << 20),
        name="finish",
    )(hat, joined)


def shards(cells, fractions, charges, influence, shells):
    parts_y = lax.axis_size("gx")
    parts_z = lax.axis_size("gy")
    hat, joined = whole(cells, fractions, charges[None], influence, shells, parts_y, parts_z)
    potential_hat, energy, virial, spectrum = finish(hat, joined)
    return (potential_hat, energy.reshape(()), virial, spectrum.reshape(SHELLS))


def solution(mesh):
    return jax.shard_map(
        shards,
        mesh=mesh,
        in_specs=(
            P(None, ("gx", "gy")),
            P(None, ("gx", "gy")),
            P(("gx", "gy")),
            P("gx", "gy", None),
            P("gx", "gy", None),
        ),
        out_specs=(P(None, "gx", "gy", None), P(), P(), P()),
        check_vma=False,
    )
```
